32 devices in a mesh: gx: 2 (over x), gy: 4 (over y, core), gz: 4 (over z).
Axes of the slice: x: 2, y: 2, z: 4, core: 2. Of those that a mesh axis runs over, the one named last changes fastest.
Arguments:
- charges: bfloat16 [8, 16, 16, 32, 128], P('gx', 'gy', 'gz'), may hold values from -6 to 6
- counts: int32 [8, 16, 16], P('gx', 'gy', 'gz'), may hold values from 32 to 128, as said below
- near_offsets: int32 [27, 3], replicated, may hold values from -1 to 1, as said below
- near_blocks: bfloat16 [27, 128, 128], replicated, may hold values from -0.109375 to 0.109375
- leaf_basis: bfloat16 [48, 128], replicated, may hold values from -0.5 to 0.5
- transfer: bfloat16 [8, 48, 48], replicated, may hold values from -0.625 to 0.625
- far_offsets: int32 [2, 32, 3], replicated, may hold values from -2 to 2, as said below
- coupling: bfloat16 [2, 32, 48, 48], replicated, may hold values from -0.15625 to 0.15625
- coarse_coupling: bfloat16 [2, 4, 4, 48, 48], replicated, may hold values from -0.3125 to 0.3125
Outputs:
- potentials: float32 [8, 16, 16, 32, 128], P('gx', 'gy', 'gz')
The draws below stay inside these ranges and needn't reach their ends.
Inputs may be any that keep to these rules, and one draw needn't show every extreme that they name: `counts`: in each device's block of 4 x 4 x 4 leaf boxes some box holds 128 points. `near_offsets`: each of the 27 offsets with components in -1, 0, 1 appears once. `far_offsets`: each level lists 32 distinct offsets whose largest component in magnitude is 2.
All inputs are finite; a program needn't handle non-finite values.
Results may differ from the reference program's by a relative error of at most 0.008.
Values may be sent and summed in bfloat16 or wider, within the bound.
A program may use at most 128 MiB of HBM per device.

```python
import jax
import jax.numpy as jnp
import numpy as np
from jax import lax

PTS = 128
RANK = 48
RHS = 32
STENCIL = 27
LIST = 32
BX = 4
BY = 4
BZ = 4
LX = 8
LY = 16
LZ = 16
CGX = 2
CGY = 4
CGZ = 4


def candidate_table():
    entries = []
    for first in range(-2, 3):
        for second in range(-2, 3):
            for third in range(-2, 3):
                if max(abs(first), abs(second), abs(third)) == 2:
                    entries.append([first, second, third])
    return np.array(entries, dtype=np.int32)


def draw_counts(key, part):
    base = jax.random.randint(jax.random.fold_in(key, 1), (LX, LY, LZ), PTS // 4, PTS + 1)
    chosen = jax.random.randint(jax.random.fold_in(key, 2), (LX // BX, LY // BY, LZ // BZ), 0, BX * BY * BZ)
    spread = jnp.repeat(jnp.repeat(jnp.repeat(chosen, BX, axis=0), BY, axis=1), BZ, axis=2)
    pos_x = (jnp.arange(LX, dtype=jnp.int32) % BX)[:, None, None]
    pos_y = (jnp.arange(LY, dtype=jnp.int32) % BY)[None, :, None]
    pos_z = (jnp.arange(LZ, dtype=jnp.int32) % BZ)[None, None, :]
    within = (pos_x * BY + pos_y) * BZ + pos_z
    return jnp.where(within == spread, PTS, base).astype(jnp.int32)


def draw_near_offsets(key, part):
    order = jax.random.permutation(jax.random.fold_in(key, 3), 27).astype(jnp.int32)
    return jnp.stack([order // 9 - 1, order // 3 % 3 - 1, order % 3 - 1], axis=1).astype(jnp.int32)


def draw_far_offsets(key, part):
    table = jnp.asarray(candidate_table())
    levels = []
    for level in range(2):
        picked = jax.random.permutation(jax.random.fold_in(key, 10 + level), table.shape[0])[:LIST]
        levels.append(table[picked])
    return jnp.stack(levels).astype(jnp.int32)


def block_levels(stream_key, extent, cuts, least, largest):
    factor_of, own = 1.0, jax.random.fold_in(stream_key, 6)
    for position, parts in cuts:
        draws = jnp.exp(jax.random.uniform(jax.random.fold_in(own, position), (parts,), jnp.float32, least / len(cuts), largest / len(cuts)))
        factor_of = factor_of * jnp.repeat(draws, extent[position] // parts).reshape([-1 if axis == position else 1 for axis in range(len(extent))])
    return factor_of


def centred(key, extent, deviation, limit, cuts=(), kind=jnp.bfloat16):
    values = jax.random.normal(key, extent, jnp.float32) * deviation
    if len(cuts) > 0:
        values = block_levels(key, extent, cuts, -0.22, 0.18) * values
    return jnp.clip(values, min=-limit, max=limit).astype(kind)


def setup_inputs(seed: int = 0) -> dict:
    arg_keys = jax.random.split(jax.random.key(seed), 10)
    charges = centred(arg_keys[0], (LX, LY, LZ, RHS, PTS), 1.0, 6.0, ((0, 2), (1, 4), (2, 4)))
    counts = draw_counts(jax.random.fold_in(arg_keys[9], 71), 0)
    near_offsets = draw_near_offsets(jax.random.fold_in(arg_keys[9], 71), 0)
    near_blocks = centred(arg_keys[3], (STENCIL, PTS, PTS), (STENCIL * PTS) ** -0.5, 0.109375)
    leaf_basis = centred(arg_keys[4], (RANK, PTS), PTS ** -0.5, 0.5)
    transfer = centred(arg_keys[5], (8, RANK, RANK), (2 * RANK) ** -0.5, 0.625)
    far_offsets = draw_far_offsets(jax.random.fold_in(arg_keys[9], 71), 0)
    coupling = centred(arg_keys[7], (2, LIST, RANK, RANK), (LIST * RANK) ** -0.5, 0.15625)
    coarse_coupling = centred(arg_keys[8], (CGX, CGY, CGZ, RANK, RANK), (CGX * CGY * CGZ * RANK // 4) ** -0.5, 0.3125)
    return {"charges": charges, "counts": counts, "near_offsets": near_offsets, "near_blocks": near_blocks, "leaf_basis": leaf_basis, "transfer": transfer, "far_offsets": far_offsets, "coupling": coupling, "coarse_coupling": coarse_coupling}


def shifted(field, offset):
    return jnp.roll(field, (-offset[0], -offset[1], -offset[2]), axis=(0, 1, 2))


def upward(moments, transfer):
    first_len, second_len, third_len, rank_count, columns = moments.shape
    split = moments.astype(jnp.float32).reshape(first_len // 2, 2, second_len // 2, 2, third_len // 2, 2, rank_count, columns)
    kids = split.transpose(0, 2, 4, 1, 3, 5, 6, 7).reshape(first_len // 2, second_len // 2, third_len // 2, 8, rank_count, columns)
    return jnp.einsum("ckj,xyzcjr->xyzkr", transfer.astype(jnp.float32), kids).astype(jnp.bfloat16)


def downward(parent, transfer):
    rounded = lax.optimization_barrier(parent.astype(jnp.bfloat16)).astype(jnp.float32)
    kids = jnp.einsum("cjk,xyzjr->xyzckr", transfer.astype(jnp.float32), rounded)
    first_len, second_len, third_len, rank_count, columns = parent.shape
    split = kids.reshape(first_len, second_len, third_len, 2, 2, 2, rank_count, columns)
    return split.transpose(0, 3, 1, 4, 2, 5, 6, 7).reshape(2 * first_len, 2 * second_len, 2 * third_len, rank_count, columns)


def couple_level(moments, offsets, matrices):
    wide = moments.astype(jnp.float32)
    mats = matrices.astype(jnp.float32)

    def step(total, index):
        moved = shifted(wide, offsets[index])
        return total + jnp.einsum("kj,xyzjr->xyzkr", mats[index], moved), None

    start = jnp.zeros(moments.shape, jnp.float32)
    total, unused = lax.scan(step, start, jnp.arange(offsets.shape[0], dtype=jnp.int32))
    return total


def coarse_level(moments, coarse_coupling):
    grid_x, grid_y, grid_z = moments.shape[:3]
    wide = moments.astype(jnp.float32)
    mats = coarse_coupling.astype(jnp.float32)

    def step(total, number):
        off_x = number // (grid_y * grid_z)
        off_y = (number // grid_z) % grid_y
        off_z = number % grid_z
        moved = jnp.roll(wide, (-off_x, -off_y, -off_z), axis=(0, 1, 2))
        return total + jnp.einsum("kj,xyzjr->xyzkr", mats[off_x, off_y, off_z], moved), None

    start = jnp.zeros(moments.shape, jnp.float32)
    total, unused = lax.scan(step, start, jnp.arange(grid_x * grid_y * grid_z, dtype=jnp.int32))
    return total


def reference(charges, counts, near_offsets, near_blocks, leaf_basis, transfer, far_offsets, coupling, coarse_coupling):
    capacity = charges.shape[4]
    live = (jnp.arange(capacity, dtype=jnp.int32) < counts[..., None]).astype(jnp.bfloat16)
    masked = charges * live[:, :, :, None, :]
    masked_wide = masked.astype(jnp.float32)
    blocks = near_blocks.astype(jnp.float32)

    def near_step(total, index):
        moved = shifted(masked_wide, near_offsets[index])
        return total + jnp.einsum("xyzrq,pq->xyzrp", moved, blocks[index]), None

    near, unused = lax.scan(near_step, jnp.zeros(charges.shape, jnp.float32), jnp.arange(near_offsets.shape[0], dtype=jnp.int32))
    basis = leaf_basis.astype(jnp.float32)
    moments_zero = jnp.einsum("kp,xyzrp->xyzkr", basis, masked_wide).astype(jnp.bfloat16)
    moments_one = upward(moments_zero, transfer)
    moments_two = upward(moments_one, transfer)
    local_zero = couple_level(moments_zero, far_offsets[0], coupling[0])
    local_one = couple_level(moments_one, far_offsets[1], coupling[1])
    local_two = coarse_level(moments_two, coarse_coupling)
    total_one = local_one + downward(local_two, transfer)
    total_zero = local_zero + downward(total_one, transfer)
    rounded = lax.optimization_barrier(total_zero.astype(jnp.bfloat16)).astype(jnp.float32)
    far = jnp.einsum("kp,xyzkr->xyzrp", basis, rounded)
    return (near + far) * live[:, :, :, None, :].astype(jnp.float32)
```

```python
import functools

import jax
import jax.numpy as jnp
from jax import lax
from jax.experimental import pallas as pl
from jax.experimental.pallas import tpu as pltpu
from jax.sharding import PartitionSpec as P

MESH = pl.DeviceIdType.MESH
AXES = ("gx", "gy", "gz")
F32 = jnp.float32
BF16 = jnp.bfloat16
NT = (((1,), (1,)), ((), ()))
NN = (((1,), (0,)), ((), ()))


def dot(a, b, dims):
    return lax.dot_general(a, b, dims, preferred_element_type=F32)


def kernel(
    sizes,
    inverse,
    counts,
    far_offsets,
    charges,
    basis,
    transfer,
    near_hbm,
    coupling_hbm,
    coarse_hbm,
    out,
    ext,
    mom,
    one,
    two,
    near_w,
    coupling_raw,
    coarse_raw,
    far_w,
    coarse_w,
    trans_w,
    basis_w,
    near_acc,
    far_acc,
    one_acc,
    local_sem,
    send_sem,
    recv_sem,
    gsend,
    grecv,
):
    bx, by, bz, rhs, pts = charges.shape
    rank = basis.shape[0]
    half = rhs // 2
    lane = pts // 2
    me = [lax.axis_index(a) for a in AXES]
    steps = coupling_raw.shape[1]
    cells = sizes[0] * sizes[1] * sizes[2]

    near_copy = pltpu.make_async_copy(near_hbm, near_w, local_sem.at[0])
    coupling_copy = pltpu.make_async_copy(coupling_hbm, coupling_raw, local_sem.at[1])
    coarse_copy = pltpu.make_async_copy(coarse_hbm, coarse_raw, local_sem.at[2])
    near_copy.start()
    coupling_copy.start()
    coarse_copy.start()

    barrier = pltpu.get_barrier_semaphore()
    peers = 0
    for axis in range(3):
        for d in range(1, sizes[axis]):
            other = lax.rem(me[axis] + d, sizes[axis])
            pl.semaphore_signal(barrier, inc=1, device_id={AXES[axis]: other}, device_id_type=MESH)
            peers += 1

    lanes = lax.broadcasted_iota(jnp.int32, (rhs, pts), 1)

    def mask_box(b, carry):
        x, y, z = b // (by * bz), b // bz % by, b % bz
        value = charges[x, y, z]
        live = (lanes < counts[x, y, z]).astype(F32).astype(BF16)
        ext[1 + x, 1 + y, 1 + z] = value * live
        return carry

    lax.fori_loop(0, bx * by * bz, mask_box, 0)
    pl.semaphore_wait(barrier, peers)

    def halo(ref, stream, width, axis, order):
        own = [(bx, by, bz), (bx, by, bz), (bx // 2, by // 2, bz // 2)][stream]
        done = order[: order.index(axis)]

        def view(start):
            index = []
            for d in range(3):
                if d == axis:
                    index.append(pl.ds(start, width))
                elif d in done:
                    index.append(pl.ds(0, ref.shape[d]))
                else:
                    index.append(pl.ds(width, own[d]))
            return ref.at[tuple(index)]

        n = own[axis]
        moves = [(n, 0, 1)]
        if ref.shape[axis] == n + 2 * width:
            moves.append((width, width + n, sizes[axis] - 1))
        copies = []
        for k, (src, dst, shift) in enumerate(moves):
            slot = (stream * 3 + axis) * 2 + k
            copies.append(
                pltpu.make_async_remote_copy(
                    src_ref=view(src),
                    dst_ref=view(dst),
                    send_sem=send_sem.at[slot],
                    recv_sem=recv_sem.at[slot],
                    device_id={AXES[axis]: lax.rem(me[axis] + shift, sizes[axis])},
                    device_id_type=MESH,
                )
            )
        return copies

    def gather(axis):
        index = [pl.ds(0, sizes[d]) if d < axis else pl.ds(me[d], 1) for d in range(3)]
        view = two.at[tuple(index)]
        copies = []
        base = sum(sizes[d] - 1 for d in range(axis))
        for d in range(1, sizes[axis]):
            copies.append(
                pltpu.make_async_remote_copy(
                    src_ref=view,
                    dst_ref=view,
                    send_sem=gsend.at[base + d - 1],
                    recv_sem=grecv.at[base + d - 1],
                    device_id={AXES[axis]: lax.rem(me[axis] + d, sizes[axis])},
                    device_id_type=MESH,
                )
            )
        return copies

    def start(copies):
        for c in copies:
            c.start()

    def arrive(copies):
        for c in copies:
            c.wait_recv()

    def gather_arrive(axis):
        base = sum(sizes[d] - 1 for d in range(axis))
        for d in range(1, sizes[axis]):
            source = lax.rem(me[axis] + sizes[axis] - d, sizes[axis])
            index = [pl.ds(0, sizes[k]) if k < axis else pl.ds(me[k], 1) for k in range(3)]
            index[axis] = pl.ds(source, 1)
            view = two.at[tuple(index)]
            pltpu.make_async_remote_copy(
                src_ref=view,
                dst_ref=view,
                send_sem=gsend.at[base + d - 1],
                recv_sem=grecv.at[base + d - 1],
                device_id={AXES[axis]: source},
                device_id_type=MESH,
            ).wait_recv()

    order_c, order_m, order_o = (0, 1, 2), (0, 2, 1), (0, 1, 2)
    ch = [halo(ext, 0, 1, a, order_c) for a in order_c]
    mo = [halo(mom, 1, 2, a, order_m) for a in order_m]
    on = [halo(one, 2, 2, a, order_o) for a in order_o]
    tw = [gather(a) for a in range(3)]

    start(ch[0])

    basis_w[...] = jnp.zeros(basis_w.shape, BF16)
    basis_w[0:rank, 0:pts] = basis[...]
    basis_w[lane : lane + rank, pts : 2 * pts] = basis[...]
    trans_w[...] = jnp.zeros(trans_w.shape, BF16)
    for c in range(8):
        trans_w[c, 0:rank, 0:rank] = transfer[c]
        trans_w[c, lane : lane + rank, lane : lane + rank] = transfer[c]

    def moments(x, carry):
        low = ext[1 + x, 1 : 1 + by, 1 : 1 + bz, 0:half].reshape(by * bz * half, pts)
        high = ext[1 + x, 1 : 1 + by, 1 : 1 + bz, half:rhs].reshape(by * bz * half, pts)
        value = dot(jnp.concatenate([low, high], axis=1), basis_w[...], NT).astype(BF16)
        mom[2 + x, 2 : 2 + by, 2 : 2 + bz] = value.reshape(by, bz, half, pts)
        return carry

    lax.fori_loop(0, bx, moments, 0)
    start(mo[0])

    hx, hy, hz = bx // 2, by // 2, bz // 2
    parents = [(a, b, c) for a in range(hx) for b in range(hy) for c in range(hz)]
    kids = [(i, j, l) for i in range(2) for j in range(2) for l in range(2)]
    total = jnp.zeros((len(parents) * half, pts), F32)
    for number, (i, j, l) in enumerate(kids):
        rows = jnp.concatenate(
            [mom[2 + 2 * a + i, 2 + 2 * b + j, 2 + 2 * c + l] for a, b, c in parents], axis=0
        )
        total = total + dot(rows, trans_w[number], NT)
    value = total.astype(BF16)
    for n, (a, b, c) in enumerate(parents):
        one[2 + a, 2 + b, 2 + c] = value[n * half : (n + 1) * half]
    start(on[0])
    total = jnp.zeros((half, pts), F32)
    for number in range(8):
        total = total + dot(value[number * half : (number + 1) * half], trans_w[number], NT)
    two[me[0], me[1], me[2]] = total.astype(BF16)
    start(tw[0])

    far_w[...] = jnp.zeros(far_w.shape, BF16)
    coarse_w[...] = jnp.zeros(coarse_w.shape, BF16)
    coupling_copy.wait()

    def build_far(t, carry):
        for level in range(2):
            for k in range(2):
                value = coupling_raw[level, 2 * t + k]
                for s in range(2):
                    col = k * pts + s * lane
                    far_w[level, t, s * lane : s * lane + rank, col : col + rank] = value
        return carry

    lax.fori_loop(0, steps // 2, build_far, 0)

    arrive(ch[0])
    start(ch[1])
    arrive(mo[0])
    start(mo[1])
    arrive(on[0])
    start(on[1])
    gather_arrive(0)
    start(tw[1])

    coarse_copy.wait()

    def build_coarse(t, carry):
        for k in range(2):
            r = 2 * t + k
            x, y, z = r // (sizes[1] * sizes[2]), r // sizes[2] % sizes[1], r % sizes[2]
            value = coarse_raw[x, y, z]
            for s in range(2):
                col = k * pts + s * lane
                coarse_w[t, s * lane : s * lane + rank, col : col + rank] = value
        return carry

    lax.fori_loop(0, cells // 2, build_coarse, 0)
    near_copy.wait()

    def window(ox, oy, oz):
        v = ext[pl.ds(ox + 1, bx), pl.ds(oy + 1, by), pl.ds(oz + 1, bz)]
        return v.reshape(bx * by * bz * rhs, pts)

    def near_weight(ox, oy, oz):
        return near_w[inverse[(ox + 1) * 9 + (oy + 1) * 3 + oz + 1]]

    near_acc[...] = dot(window(0, 0, 0), near_weight(0, 0, 0), NT)

    def near_pair(first, second):
        rows = jnp.concatenate([window(*first), window(*second)], axis=1)
        mats = jnp.concatenate([near_weight(*first), near_weight(*second)], axis=1)
        near_acc[...] += dot(rows, mats, NT)

    near_pair((-1, 0, 0), (1, 0, 0))

    arrive(ch[1])
    start(ch[2])
    arrive(mo[1])
    start(mo[2])
    arrive(on[1])
    start(on[2])
    gather_arrive(1)
    start(tw[2])

    def near_middle(t, carry):
        near_pair((t - 1, -1, 0), (t - 1, 1, 0))
        return carry

    lax.fori_loop(0, 3, near_middle, 0)

    arrive(ch[2])

    def near_last(t, carry):
        near_pair((t // 3 - 1, t % 3 - 1, -1), (t // 3 - 1, t % 3 - 1, 1))
        return carry

    lax.fori_loop(0, 9, near_last, 0)

    gather_arrive(2)

    def coarse_step(t, total):
        rows = []
        for k in range(2):
            r = 2 * t + k
            x, y, z = r // (sizes[1] * sizes[2]), r // sizes[2] % sizes[1], r % sizes[2]
            rows.append(
                two[
                    lax.rem(me[0] + x, sizes[0]),
                    lax.rem(me[1] + y, sizes[1]),
                    lax.rem(me[2] + z, sizes[2]),
                ]
            )
        return total + dot(jnp.concatenate(rows, axis=1), coarse_w[t], NT)

    local_two = lax.fori_loop(0, cells // 2, coarse_step, jnp.zeros((half, pts), F32))

    arrive(on[2])

    def far_window(ref, level, e, count):
        ox, oy, oz = (far_offsets[level, e, d] + 2 for d in range(3))
        planes = []
        for i in range(count[0]):
            x = lax.rem(ox + i, ref.shape[0])
            v = ref[x, pl.ds(oy, count[1]), pl.ds(oz, count[2])]
            planes.append(v.reshape(count[1] * count[2] * half, pts))
        return jnp.concatenate(planes, axis=0)

    def far_product(ref, level, t, count):
        rows = [far_window(ref, level, 2 * t + k, count) for k in range(2)]
        return dot(jnp.concatenate(rows, axis=1), far_w[level, t], NT)

    one_acc[...] = jnp.zeros(one_acc.shape, F32)

    def far_one(t, carry):
        one_acc[...] += far_product(one, 1, t, (hx, hy, hz))
        return carry

    lax.fori_loop(0, steps // 2, far_one, 0)

    rounded = local_two.astype(BF16)
    for number in range(8):
        rows = slice(number * half, (number + 1) * half)
        one_acc[rows, :] += dot(rounded, trans_w[number], NN)

    rounded = one_acc[...].astype(BF16)
    for number, (i, j, l) in enumerate(kids):
        value = dot(rounded, trans_w[number], NN)
        for n, (a, b, c) in enumerate(parents):
            box = ((2 * a + i) * by + 2 * b + j) * bz + 2 * c + l
            far_acc[box * half : (box + 1) * half, :] = value[n * half : (n + 1) * half]

    arrive(mo[2])

    def far_zero(t, carry):
        far_acc[...] += far_product(mom, 0, t, (bx, by, bz))
        return carry

    lax.fori_loop(0, steps // 2, far_zero, 0)

    def finish(x, carry):
        span = by * bz * half
        rows = far_acc[pl.ds(pl.multiple_of(x * span, span), span), :].astype(BF16)
        value = dot(rows, basis_w[...], NN)
        for b in range(by * bz):
            y, z = b // bz, b % bz
            live = (lanes < counts[x, y, z]).astype(F32)
            far = jnp.concatenate(
                [
                    value[b * half : (b + 1) * half, 0:pts],
                    value[b * half : (b + 1) * half, pts : 2 * pts],
                ],
                axis=0,
            )
            at = pl.multiple_of((x * by * bz + b) * rhs, rhs)
            out[x, y, z] = (near_acc[pl.ds(at, rhs), :] + far) * live
        return carry

    lax.fori_loop(0, bx, finish, 0)

    for group in ch + mo + on + tw:
        for c in group:
            c.wait_send()


def body(
    sizes,
    charges,
    counts,
    near_offsets,
    near_blocks,
    leaf_basis,
    transfer,
    far_offsets,
    coupling,
    coarse_coupling,
):
    bx, by, bz, rhs, pts = charges.shape
    half = rhs // 2
    stencil = near_offsets.shape[0]
    code = (near_offsets[:, 0] + 1) * 9 + (near_offsets[:, 1] + 1) * 3 + near_offsets[:, 2] + 1
    number = jnp.arange(stencil, dtype=jnp.int32)
    inverse = jnp.sum(
        jnp.where(code[None, :] == number[:, None], number[None, :], 0), axis=1, dtype=jnp.int32
    )
    boxes = bx * by * bz
    hx, hy, hz = bx // 2, by // 2, bz // 2
    one_x = hx + 2 if sizes[0] * hx == hx + 2 else hx + 4
    levels, steps = coupling.shape[:2]
    cells = sizes[0] * sizes[1] * sizes[2]
    peers = sum(sizes) - 3
    smem = pl.BlockSpec(memory_space=pltpu.SMEM)
    vmem = pl.BlockSpec(memory_space=pltpu.VMEM)
    hbm = pl.BlockSpec(memory_space=pl.ANY)
    return pl.pallas_call(
        functools.partial(kernel, sizes),
        out_shape=jax.ShapeDtypeStruct(charges.shape, F32),
        in_specs=[smem, smem, smem, vmem, vmem, vmem, hbm, hbm, hbm],
        out_specs=vmem,
        scratch_shapes=[
            pltpu.VMEM((bx + 2, by + 2, bz + 2, rhs, pts), BF16),
            pltpu.VMEM((bx + 4, by + 4, bz + 4, half, pts), BF16),
            pltpu.VMEM((one_x, hy + 4, hz + 4, half, pts), BF16),
            pltpu.VMEM(tuple(sizes) + (half, pts), BF16),
            pltpu.VMEM(near_blocks.shape, BF16),
            pltpu.VMEM(coupling.shape, BF16),
            pltpu.VMEM(coarse_coupling.shape, BF16),
            pltpu.VMEM((levels, steps // 2, pts, 2 * pts), BF16),
            pltpu.VMEM((cells // 2, pts, 2 * pts), BF16),
            pltpu.VMEM((8, pts, pts), BF16),
            pltpu.VMEM((pts, 2 * pts), BF16),
            pltpu.VMEM((boxes * rhs, pts), F32),
            pltpu.VMEM((boxes * half, pts), F32),
            pltpu.VMEM((hx * hy * hz * half, pts), F32),
            pltpu.SemaphoreType.DMA((3,)),
            pltpu.SemaphoreType.DMA((18,)),
            pltpu.SemaphoreType.DMA((18,)),
            pltpu.SemaphoreType.DMA((peers,)),
            pltpu.SemaphoreType.DMA((peers,)),
        ],
        compiler_params=pltpu.CompilerParams(
            collective_id=0, has_side_effects=True, vmem_limit_bytes=56 * 1024 * 1024
        ),
    )(
        inverse,
        counts,
        far_offsets,
        charges,
        leaf_basis,
        transfer,
        near_blocks,
        coupling,
        coarse_coupling,
    )


def solution(mesh):
    sizes = tuple(mesh.shape[a] for a in AXES)
    in_specs = (
        P("gx", "gy", "gz", None, None),
        P("gx", "gy", "gz"),
        P(),
        P(),
        P(),
        P(),
        P(),
        P(),
        P(),
    )
    out_specs = P("gx", "gy", "gz", None, None)
    return jax.shard_map(
        functools.partial(body, sizes),
        mesh=mesh,
        in_specs=in_specs,
        out_specs=out_specs,
        check_vma=False,
    )
```

```python
import functools

import jax
import jax.numpy as jnp
from jax import lax
from jax.experimental import pallas as pl
from jax.experimental.pallas import tpu as pltpu
from jax.sharding import PartitionSpec as P

MESH = pl.DeviceIdType.MESH
AXES = ("gx", "gy", "gz")
F32 = jnp.float32
BF16 = jnp.bfloat16
NT = (((1,), (1,)), ((), ()))
NN = (((1,), (0,)), ((), ()))


def dot(a, b, dims):
    return lax.dot_general(a, b, dims, preferred_element_type=F32)


def kernel(
    sizes,
    near_offsets,
    counts,
    far_offsets,
    charges,
    basis,
    transfer,
    near_hbm,
    coupling_hbm,
    coarse_hbm,
    out,
    ext,
    mom,
    one,
    two,
    near_w,
    coupling_raw,
    coarse_raw,
    far_w,
    coarse_w,
    trans_w,
    basis_w,
    near_acc,
    far_acc,
    one_acc,
    code,
    inverse,
    local_sem,
    send_sem,
    recv_sem,
    gsend,
    grecv,
):
    bx, by, bz, rhs, pts = charges.shape
    rank = basis.shape[0]
    half = rhs // 2
    lane = pts // 2
    me = [lax.axis_index(a) for a in AXES]
    steps = coupling_raw.shape[1]
    cells = sizes[0] * sizes[1] * sizes[2]

    near_copy = pltpu.make_async_copy(near_hbm, near_w, local_sem.at[0])
    coupling_copy = pltpu.make_async_copy(coupling_hbm, coupling_raw, local_sem.at[1])
    coarse_copy = pltpu.make_async_copy(coarse_hbm, coarse_raw, local_sem.at[2])
    near_copy.start()
    coupling_copy.start()
    coarse_copy.start()

    barrier = pltpu.get_barrier_semaphore()
    peers = 0
    for axis in range(3):
        for d in range(1, sizes[axis]):
            other = lax.rem(me[axis] + d, sizes[axis])
            pl.semaphore_signal(barrier, inc=1, device_id={AXES[axis]: other}, device_id_type=MESH)
            peers += 1

    lanes = lax.broadcasted_iota(jnp.int32, (rhs, pts), 1)

    def mask_box(b, carry):
        x, y, z = b // (by * bz), b // bz % by, b % bz
        value = charges[x, y, z]
        live = (lanes < counts[x, y, z]).astype(F32).astype(BF16)
        ext[1 + x, 1 + y, 1 + z] = value * live
        return carry

    lax.fori_loop(0, bx * by * bz, mask_box, 0)
    pl.semaphore_wait(barrier, peers)

    def halo(ref, stream, width, order):
        own = [(bx, by, bz), (bx, by, bz), (bx // 2, by // 2, bz // 2)][stream]
        high = [ref.shape[d] == own[d] + 2 * width for d in range(3)]
        part = {
            "o": lambda d: pl.ds(width, own[d]),
            "l": lambda d: pl.ds(0, width),
            "h": lambda d: pl.ds(width + own[d], width),
            "f": lambda d: pl.ds(0, ref.shape[d]),
        }
        first, second, third = order
        plans = [("A", first, {}), ("B", second, {first: "o"})]
        plans += [("Bs", second, {first: side}) for side in "lh"]
        plans += [("C", third, {first: "o", second: "o"})]
        plans += [("Cs", third, {first: side, second: "o"}) for side in "lh"]
        plans += [("Cf", third, {first: "f", second: side}) for side in "lh"]
        groups = {"A": [], "B": [], "Bs": [], "C": [], "Cs": [], "Cf": []}
        slot = stream * 18
        for name, axis, fixed in plans:
            if any(side == "h" and not high[d] for d, side in fixed.items()):
                continue

            def view(start):
                index = [part[fixed.get(d, "o")](d) for d in range(3)]
                index[axis] = pl.ds(start, width)
                return ref.at[tuple(index)]

            n = own[axis]
            moves = [(n, 0, 1)]
            if high[axis]:
                moves.append((width, width + n, sizes[axis] - 1))
            for src, dst, shift in moves:
                groups[name].append(
                    pltpu.make_async_remote_copy(
                        src_ref=view(src),
                        dst_ref=view(dst),
                        send_sem=send_sem.at[slot],
                        recv_sem=recv_sem.at[slot],
                        device_id={AXES[axis]: lax.rem(me[axis] + shift, sizes[axis])},
                        device_id_type=MESH,
                    )
                )
                slot += 1
        return groups

    def gather(axis):
        index = [pl.ds(0, sizes[d]) if d < axis else pl.ds(me[d], 1) for d in range(3)]
        view = two.at[tuple(index)]
        copies = []
        base = sum(sizes[d] - 1 for d in range(axis))
        for d in range(1, sizes[axis]):
            copies.append(
                pltpu.make_async_remote_copy(
                    src_ref=view,
                    dst_ref=view,
                    send_sem=gsend.at[base + d - 1],
                    recv_sem=grecv.at[base + d - 1],
                    device_id={AXES[axis]: lax.rem(me[axis] + d, sizes[axis])},
                    device_id_type=MESH,
                )
            )
        return copies

    def start(copies):
        for c in copies:
            c.start()

    def arrive(copies):
        for c in copies:
            c.wait_recv()

    def gather_arrive(axis):
        base = sum(sizes[d] - 1 for d in range(axis))
        for d in range(1, sizes[axis]):
            source = lax.rem(me[axis] + sizes[axis] - d, sizes[axis])
            index = [pl.ds(0, sizes[k]) if k < axis else pl.ds(me[k], 1) for k in range(3)]
            index[axis] = pl.ds(source, 1)
            view = two.at[tuple(index)]
            pltpu.make_async_remote_copy(
                src_ref=view,
                dst_ref=view,
                send_sem=gsend.at[base + d - 1],
                recv_sem=grecv.at[base + d - 1],
                device_id={AXES[axis]: source},
                device_id_type=MESH,
            ).wait_recv()

    ch = halo(ext, 0, 1, (0, 1, 2))
    mo = halo(mom, 1, 2, (0, 2, 1))
    on = halo(one, 2, 2, (0, 1, 2))
    tw = [gather(a) for a in range(3)]

    def begin(groups):
        for name in ("A", "B", "C"):
            start(groups[name])

    def middle(groups):
        arrive(groups["A"])
        start(groups["Bs"])
        start(groups["Cs"])

    def corner(groups):
        arrive(groups["B"])
        arrive(groups["Bs"])
        start(groups["Cf"])

    def ending(groups):
        for name in ("C", "Cs", "Cf"):
            arrive(groups[name])

    begin(ch)

    basis_w[...] = jnp.zeros(basis_w.shape, BF16)
    basis_w[0:rank, 0:pts] = basis[...]
    basis_w[lane : lane + rank, pts : 2 * pts] = basis[...]
    trans_w[...] = jnp.zeros(trans_w.shape, BF16)
    for c in range(8):
        trans_w[c, 0:rank, 0:rank] = transfer[c]
        trans_w[c, lane : lane + rank, lane : lane + rank] = transfer[c]

    def moments(x, carry):
        low = ext[1 + x, 1 : 1 + by, 1 : 1 + bz, 0:half].reshape(by * bz * half, pts)
        high = ext[1 + x, 1 : 1 + by, 1 : 1 + bz, half:rhs].reshape(by * bz * half, pts)
        value = dot(jnp.concatenate([low, high], axis=1), basis_w[...], NT).astype(BF16)
        mom[2 + x, 2 : 2 + by, 2 : 2 + bz] = value.reshape(by, bz, half, pts)
        return carry

    lax.fori_loop(0, bx, moments, 0)
    begin(mo)

    hx, hy, hz = bx // 2, by // 2, bz // 2
    parents = [(a, b, c) for a in range(hx) for b in range(hy) for c in range(hz)]
    kids = [(i, j, l) for i in range(2) for j in range(2) for l in range(2)]
    total = jnp.zeros((len(parents) * half, pts), F32)
    for number, (i, j, l) in enumerate(kids):
        rows = jnp.concatenate(
            [mom[2 + 2 * a + i, 2 + 2 * b + j, 2 + 2 * c + l] for a, b, c in parents], axis=0
        )
        total = total + dot(rows, trans_w[number], NT)
    value = total.astype(BF16)
    for n, (a, b, c) in enumerate(parents):
        one[2 + a, 2 + b, 2 + c] = value[n * half : (n + 1) * half]
    begin(on)
    total = jnp.zeros((half, pts), F32)
    for number in range(8):
        total = total + dot(value[number * half : (number + 1) * half], trans_w[number], NT)
    two[me[0], me[1], me[2]] = total.astype(BF16)
    start(tw[0])

    stencil = near_offsets.shape[1]
    for number in range(stencil):
        x, y, z = (near_offsets[d, number] + 1 for d in range(3))
        code[number] = x * 9 + y * 3 + z

    def invert(c, carry):
        found = jnp.int32(0)
        for number in range(stencil):
            found = found + jnp.where(code[number] == c, number, 0)
        inverse[c] = jnp.minimum(found, stencil - 1)
        return carry

    lax.fori_loop(0, stencil, invert, 0)
    far_w[...] = jnp.zeros(far_w.shape, BF16)
    coarse_w[...] = jnp.zeros(coarse_w.shape, BF16)
    coupling_copy.wait()

    def build_far(t, carry):
        for level in range(2):
            for k in range(4):
                value = coupling_raw[level, 4 * t + k]
                for s in range(2):
                    col = k * pts + s * lane
                    far_w[level, t, s * lane : s * lane + rank, col : col + rank] = value
        return carry

    lax.fori_loop(0, steps // 4, build_far, 0)

    middle(ch)
    middle(mo)
    middle(on)
    gather_arrive(0)
    start(tw[1])

    coarse_copy.wait()

    def build_coarse(t, carry):
        for k in range(2):
            r = 2 * t + k
            x, y, z = r // (sizes[1] * sizes[2]), r // sizes[2] % sizes[1], r % sizes[2]
            value = coarse_raw[x, y, z]
            for s in range(2):
                col = k * pts + s * lane
                coarse_w[t, s * lane : s * lane + rank, col : col + rank] = value
        return carry

    lax.fori_loop(0, cells // 2, build_coarse, 0)
    near_copy.wait()

    def window(ox, oy, oz):
        v = ext[pl.ds(ox + 1, bx), pl.ds(oy + 1, by), pl.ds(oz + 1, bz)]
        return v.reshape(bx * by * bz * rhs, pts)

    def near_weight(ox, oy, oz):
        return near_w[inverse[(ox + 1) * 9 + (oy + 1) * 3 + oz + 1]]

    near_acc[...] = dot(window(0, 0, 0), near_weight(0, 0, 0), NT)

    def near_pair(first, second):
        rows = jnp.concatenate([window(*first), window(*second)], axis=1)
        mats = jnp.concatenate([near_weight(*first), near_weight(*second)], axis=1)
        near_acc[...] += dot(rows, mats, NT)

    near_pair((-1, 0, 0), (1, 0, 0))

    corner(ch)
    corner(mo)
    corner(on)
    gather_arrive(1)
    start(tw[2])

    def near_middle(t, carry):
        near_pair((t - 1, -1, 0), (t - 1, 1, 0))
        return carry

    lax.fori_loop(0, 3, near_middle, 0)

    ending(ch)

    def near_last(t, carry):
        near_pair((t // 3 - 1, t % 3 - 1, -1), (t // 3 - 1, t % 3 - 1, 1))
        return carry

    lax.fori_loop(0, 9, near_last, 0)

    gather_arrive(2)

    def coarse_step(t, total):
        rows = []
        for k in range(2):
            r = 2 * t + k
            x, y, z = r // (sizes[1] * sizes[2]), r // sizes[2] % sizes[1], r % sizes[2]
            rows.append(
                two[
                    lax.rem(me[0] + x, sizes[0]),
                    lax.rem(me[1] + y, sizes[1]),
                    lax.rem(me[2] + z, sizes[2]),
                ]
            )
        return total + dot(jnp.concatenate(rows, axis=1), coarse_w[t], NT)

    local_two = lax.fori_loop(0, cells // 2, coarse_step, jnp.zeros((half, pts), F32))

    ending(on)

    def far_window(ref, level, e, count):
        ox, oy, oz = (far_offsets[d, level, e] + 2 for d in range(3))
        planes = []
        for i in range(count[0]):
            x = lax.rem(ox + i, ref.shape[0])
            v = ref[x, pl.ds(oy, count[1]), pl.ds(oz, count[2])]
            planes.append(v.reshape(count[1] * count[2] * half, pts))
        return jnp.concatenate(planes, axis=0)

    def far_product(ref, level, t, count):
        rows = [far_window(ref, level, 4 * t + k, count) for k in range(4)]
        return dot(jnp.concatenate(rows, axis=1), far_w[level, t], NT)

    one_acc[...] = jnp.zeros(one_acc.shape, F32)

    def far_one(t, carry):
        one_acc[...] += far_product(one, 1, t, (hx, hy, hz))
        return carry

    lax.fori_loop(0, steps // 4, far_one, 0)

    rounded = local_two.astype(BF16)
    for number in range(8):
        rows = slice(number * half, (number + 1) * half)
        one_acc[rows, :] += dot(rounded, trans_w[number], NN)

    rounded = one_acc[...].astype(BF16)
    for number, (i, j, l) in enumerate(kids):
        value = dot(rounded, trans_w[number], NN)
        for n, (a, b, c) in enumerate(parents):
            box = ((2 * a + i) * by + 2 * b + j) * bz + 2 * c + l
            far_acc[box * half : (box + 1) * half, :] = value[n * half : (n + 1) * half]

    ending(mo)

    def far_zero(t, carry):
        far_acc[...] += far_product(mom, 0, t, (bx, by, bz))
        return carry

    lax.fori_loop(0, steps // 4, far_zero, 0)

    def finish(x, carry):
        span = by * bz * half
        rows = far_acc[pl.ds(pl.multiple_of(x * span, span), span), :].astype(BF16)
        value = dot(rows, basis_w[...], NN)
        for b in range(by * bz):
            y, z = b // bz, b % bz
            live = (lanes < counts[x, y, z]).astype(F32)
            far = jnp.concatenate(
                [
                    value[b * half : (b + 1) * half, 0:pts],
                    value[b * half : (b + 1) * half, pts : 2 * pts],
                ],
                axis=0,
            )
            at = pl.multiple_of((x * by * bz + b) * rhs, rhs)
            out[x, y, z] = (near_acc[pl.ds(at, rhs), :] + far) * live
        return carry

    lax.fori_loop(0, bx, finish, 0)

    groups = list(ch.values()) + list(mo.values()) + list(on.values()) + tw
    for group in groups:
        for c in group:
            c.wait_send()


def body(
    sizes,
    charges,
    counts,
    near_offsets,
    near_blocks,
    leaf_basis,
    transfer,
    far_offsets,
    coupling,
    coarse_coupling,
):
    bx, by, bz, rhs, pts = charges.shape
    half = rhs // 2
    stencil = near_offsets.shape[0]
    boxes = bx * by * bz
    hx, hy, hz = bx // 2, by // 2, bz // 2
    one_x = hx + 2 if sizes[0] * hx == hx + 2 else hx + 4
    levels, steps = coupling.shape[:2]
    cells = sizes[0] * sizes[1] * sizes[2]
    peers = sum(sizes) - 3
    smem = pl.BlockSpec(memory_space=pltpu.SMEM)
    vmem = pl.BlockSpec(memory_space=pltpu.VMEM)
    hbm = pl.BlockSpec(memory_space=pl.ANY)
    return pl.pallas_call(
        functools.partial(kernel, sizes),
        out_shape=jax.ShapeDtypeStruct(charges.shape, F32),
        in_specs=[smem, smem, smem, vmem, vmem, vmem, hbm, hbm, hbm],
        out_specs=vmem,
        scratch_shapes=[
            pltpu.VMEM((bx + 2, by + 2, bz + 2, rhs, pts), BF16),
            pltpu.VMEM((bx + 4, by + 4, bz + 4, half, pts), BF16),
            pltpu.VMEM((one_x, hy + 4, hz + 4, half, pts), BF16),
            pltpu.VMEM(tuple(sizes) + (half, pts), BF16),
            pltpu.VMEM(near_blocks.shape, BF16),
            pltpu.VMEM(coupling.shape, BF16),
            pltpu.VMEM(coarse_coupling.shape, BF16),
            pltpu.VMEM((levels, steps // 4, pts, 4 * pts), BF16),
            pltpu.VMEM((cells // 2, pts, 2 * pts), BF16),
            pltpu.VMEM((8, pts, pts), BF16),
            pltpu.VMEM((pts, 2 * pts), BF16),
            pltpu.VMEM((boxes * rhs, pts), F32),
            pltpu.VMEM((boxes * half, pts), F32),
            pltpu.VMEM((hx * hy * hz * half, pts), F32),
            pltpu.SMEM((stencil,), jnp.int32),
            pltpu.SMEM((stencil,), jnp.int32),
            pltpu.SemaphoreType.DMA((3,)),
            pltpu.SemaphoreType.DMA((54,)),
            pltpu.SemaphoreType.DMA((54,)),
            pltpu.SemaphoreType.DMA((peers,)),
            pltpu.SemaphoreType.DMA((peers,)),
        ],
        compiler_params=pltpu.CompilerParams(
            collective_id=0, has_side_effects=True, vmem_limit_bytes=56 * 1024 * 1024
        ),
    )(
        near_offsets.T,
        counts,
        far_offsets.transpose(2, 0, 1),
        charges,
        leaf_basis,
        transfer,
        near_blocks,
        coupling,
        coarse_coupling,
    )


def solution(mesh):
    sizes = tuple(mesh.shape[a] for a in AXES)
    in_specs = (
        P("gx", "gy", "gz", None, None),
        P("gx", "gy", "gz"),
        P(),
        P(),
        P(),
        P(),
        P(),
        P(),
        P(),
    )
    out_specs = P("gx", "gy", "gz", None, None)
    return jax.shard_map(
        functools.partial(body, sizes),
        mesh=mesh,
        in_specs=in_specs,
        out_specs=out_specs,
        check_vma=False,
    )
```

```python
import functools

import jax
import jax.numpy as jnp
from jax import lax
from jax.experimental import pallas as pl
from jax.experimental.pallas import tpu as pltpu
from jax.sharding import PartitionSpec as P

MESH = pl.DeviceIdType.MESH
AXES = ("gx", "gy", "gz")
F32 = jnp.float32
BF16 = jnp.bfloat16
NT = (((1,), (1,)), ((), ()))
NN = (((1,), (0,)), ((), ()))


def dot(a, b, dims):
    return lax.dot_general(a, b, dims, preferred_element_type=F32)


def kernel(
    sizes,
    near_offsets,
    counts,
    far_offsets,
    charges,
    basis,
    transfer,
    near_hbm,
    coupling_hbm,
    coarse_hbm,
    out,
    ext,
    mom,
    one,
    two,
    near_w,
    coupling_raw,
    coarse_raw,
    far_w,
    coarse_w,
    trans_w,
    basis_w,
    near_acc,
    far_acc,
    one_acc,
    code,
    inverse,
    local_sem,
    send_sem,
    recv_sem,
    gsend,
    grecv,
):
    bx, by, bz, rhs, pts = charges.shape
    rank = basis.shape[0]
    half = rhs // 2
    lane = pts // 2
    me = [lax.axis_index(a) for a in AXES]
    steps = coupling_raw.shape[1]
    cells = sizes[0] * sizes[1] * sizes[2]

    near_copy = pltpu.make_async_copy(near_hbm, near_w, local_sem.at[0])
    coupling_copy = pltpu.make_async_copy(coupling_hbm, coupling_raw, local_sem.at[1])
    coarse_copy = pltpu.make_async_copy(coarse_hbm, coarse_raw, local_sem.at[2])
    near_copy.start()
    coupling_copy.start()
    coarse_copy.start()

    barrier = pltpu.get_barrier_semaphore()
    peers = 0
    for axis in range(3):
        for d in range(1, sizes[axis]):
            other = lax.rem(me[axis] + d, sizes[axis])
            pl.semaphore_signal(barrier, inc=1, device_id={AXES[axis]: other}, device_id_type=MESH)
            peers += 1

    lanes = lax.broadcasted_iota(jnp.int32, (rhs, pts), 1)

    def mask_box(b, carry):
        x, y, z = b // (by * bz), b // bz % by, b % bz
        value = charges[x, y, z]
        live = (lanes < counts[x, y, z]).astype(F32).astype(BF16)
        ext[1 + x, 1 + y, 1 + z] = value * live
        return carry

    lax.fori_loop(0, bx * by * bz, mask_box, 0)

    def halo(ref, stream, width, order):
        own = [(bx, by, bz), (bx, by, bz), (bx // 2, by // 2, bz // 2)][stream]
        high = [ref.shape[d] == own[d] + 2 * width for d in range(3)]
        part = {
            "o": lambda d: pl.ds(width, own[d]),
            "l": lambda d: pl.ds(0, width),
            "h": lambda d: pl.ds(width + own[d], width),
            "f": lambda d: pl.ds(0, ref.shape[d]),
        }
        first, second, third = order
        plans = [("A", first, {}), ("B", second, {first: "o"})]
        plans += [("Bs", second, {first: side}) for side in "lh"]
        plans += [("C", third, {first: "o", second: "o"})]
        plans += [("Cs", third, {first: side, second: "o"}) for side in "lh"]
        plans += [("Cf", third, {first: "f", second: side}) for side in "lh"]
        groups = {"A": [], "B": [], "Bs": [], "C": [], "Cs": [], "Cf": []}
        slot = stream * 18
        for name, axis, fixed in plans:
            if any(side == "h" and not high[d] for d, side in fixed.items()):
                continue

            def view(start):
                index = [part[fixed.get(d, "o")](d) for d in range(3)]
                index[axis] = pl.ds(start, width)
                return ref.at[tuple(index)]

            n = own[axis]
            moves = [(n, 0, 1)]
            if high[axis]:
                moves.append((width, width + n, sizes[axis] - 1))
            for src, dst, shift in moves:
                groups[name].append(
                    pltpu.make_async_remote_copy(
                        src_ref=view(src),
                        dst_ref=view(dst),
                        send_sem=send_sem.at[slot],
                        recv_sem=recv_sem.at[slot],
                        device_id={AXES[axis]: lax.rem(me[axis] + shift, sizes[axis])},
                        device_id_type=MESH,
                    )
                )
                slot += 1
        return groups

    def gather(axis):
        index = [pl.ds(0, sizes[d]) if d < axis else pl.ds(me[d], 1) for d in range(3)]
        view = two.at[tuple(index)]
        copies = []
        base = sum(sizes[d] - 1 for d in range(axis))
        for d in range(1, sizes[axis]):
            copies.append(
                pltpu.make_async_remote_copy(
                    src_ref=view,
                    dst_ref=view,
                    send_sem=gsend.at[base + d - 1],
                    recv_sem=grecv.at[base + d - 1],
                    device_id={AXES[axis]: lax.rem(me[axis] + d, sizes[axis])},
                    device_id_type=MESH,
                )
            )
        return copies

    def start(copies):
        for c in copies:
            c.start()

    def arrive(copies):
        for c in copies:
            c.wait_recv()

    def gather_arrive(axis):
        base = sum(sizes[d] - 1 for d in range(axis))
        for d in range(1, sizes[axis]):
            source = lax.rem(me[axis] + sizes[axis] - d, sizes[axis])
            index = [pl.ds(0, sizes[k]) if k < axis else pl.ds(me[k], 1) for k in range(3)]
            index[axis] = pl.ds(source, 1)
            view = two.at[tuple(index)]
            pltpu.make_async_remote_copy(
                src_ref=view,
                dst_ref=view,
                send_sem=gsend.at[base + d - 1],
                recv_sem=grecv.at[base + d - 1],
                device_id={AXES[axis]: source},
                device_id_type=MESH,
            ).wait_recv()

    ch = halo(ext, 0, 1, (0, 1, 2))
    mo = halo(mom, 1, 2, (0, 2, 1))
    on = halo(one, 2, 2, (0, 1, 2))
    tw = [gather(a) for a in range(3)]

    def begin(groups):
        for name in ("A", "B", "C"):
            start(groups[name])

    def middle(groups):
        for k, copy in enumerate(groups["A"]):
            copy.wait_recv()
            start(groups["Bs"][2 * k : 2 * k + 2])
            start(groups["Cs"][2 * k : 2 * k + 2])

    def corner(groups):
        for k in range(2):
            arrive(groups["B"][k::2])
            arrive(groups["Bs"][k::2])
            start(groups["Cf"][2 * k : 2 * k + 2])

    def ending(groups):
        for name in ("C", "Cs", "Cf"):
            arrive(groups[name])

    basis_w[...] = jnp.zeros(basis_w.shape, BF16)
    basis_w[0:rank, 0:pts] = basis[...]
    basis_w[lane : lane + rank, pts : 2 * pts] = basis[...]
    trans_w[...] = jnp.zeros(trans_w.shape, BF16)
    for c in range(8):
        trans_w[c, 0:rank, 0:rank] = transfer[c]
        trans_w[c, lane : lane + rank, lane : lane + rank] = transfer[c]

    def moments(x, carry):
        low = ext[1 + x, 1 : 1 + by, 1 : 1 + bz, 0:half].reshape(by * bz * half, pts)
        high = ext[1 + x, 1 : 1 + by, 1 : 1 + bz, half:rhs].reshape(by * bz * half, pts)
        value = dot(jnp.concatenate([low, high], axis=1), basis_w[...], NT).astype(BF16)
        mom[2 + x, 2 : 2 + by, 2 : 2 + bz] = value.reshape(by, bz, half, pts)
        return carry

    lax.fori_loop(0, bx, moments, 0)
    pl.semaphore_wait(barrier, peers)
    begin(mo)

    hx, hy, hz = bx // 2, by // 2, bz // 2
    parents = [(a, b, c) for a in range(hx) for b in range(hy) for c in range(hz)]
    kids = [(i, j, l) for i in range(2) for j in range(2) for l in range(2)]
    total = jnp.zeros((len(parents) * half, pts), F32)
    for number, (i, j, l) in enumerate(kids):
        rows = jnp.concatenate(
            [mom[2 + 2 * a + i, 2 + 2 * b + j, 2 + 2 * c + l] for a, b, c in parents], axis=0
        )
        total = total + dot(rows, trans_w[number], NT)
    value = total.astype(BF16)
    for n, (a, b, c) in enumerate(parents):
        one[2 + a, 2 + b, 2 + c] = value[n * half : (n + 1) * half]
    begin(on)
    total = jnp.zeros((half, pts), F32)
    for number in range(8):
        total = total + dot(value[number * half : (number + 1) * half], trans_w[number], NT)
    two[me[0], me[1], me[2]] = total.astype(BF16)
    start(tw[0])
    begin(ch)

    stencil = near_offsets.shape[1]
    for number in range(stencil):
        x, y, z = (near_offsets[d, number] + 1 for d in range(3))
        code[number] = x * 9 + y * 3 + z

    def invert(c, carry):
        found = jnp.int32(0)
        for number in range(stencil):
            found = found + jnp.where(code[number] == c, number, 0)
        inverse[c] = jnp.minimum(found, stencil - 1)
        return carry

    lax.fori_loop(0, stencil, invert, 0)
    far_w[...] = jnp.zeros(far_w.shape, BF16)
    coarse_w[...] = jnp.zeros(coarse_w.shape, BF16)
    coupling_copy.wait()

    def build_far(t, carry):
        for level in range(2):
            for k in range(4):
                value = coupling_raw[level, 4 * t + k]
                for s in range(2):
                    col = k * pts + s * lane
                    far_w[level, t, s * lane : s * lane + rank, col : col + rank] = value
        return carry

    lax.fori_loop(0, steps // 4, build_far, 0)

    middle(mo)
    middle(on)
    gather_arrive(0)
    start(tw[1])

    coarse_copy.wait()

    def build_coarse(t, carry):
        for k in range(2):
            r = 2 * t + k
            x, y, z = r // (sizes[1] * sizes[2]), r // sizes[2] % sizes[1], r % sizes[2]
            value = coarse_raw[x, y, z]
            for s in range(2):
                col = k * pts + s * lane
                coarse_w[t, s * lane : s * lane + rank, col : col + rank] = value
        return carry

    lax.fori_loop(0, cells // 2, build_coarse, 0)
    near_copy.wait()

    def window(ox, oy, oz):
        v = ext[pl.ds(ox + 1, bx), pl.ds(oy + 1, by), pl.ds(oz + 1, bz)]
        return v.reshape(bx * by * bz * rhs, pts)

    def near_weight(ox, oy, oz):
        return near_w[inverse[(ox + 1) * 9 + (oy + 1) * 3 + oz + 1]]

    near_acc[...] = dot(window(0, 0, 0), near_weight(0, 0, 0), NT)

    def near_pair(first, second):
        rows = jnp.concatenate([window(*first), window(*second)], axis=1)
        mats = jnp.concatenate([near_weight(*first), near_weight(*second)], axis=1)
        near_acc[...] += dot(rows, mats, NT)

    gather_arrive(1)
    start(tw[2])
    corner(on)
    corner(mo)
    middle(ch)
    near_pair((-1, 0, 0), (1, 0, 0))
    corner(ch)

    def near_middle(t, carry):
        near_pair((t - 1, -1, 0), (t - 1, 1, 0))
        return carry

    lax.fori_loop(0, 3, near_middle, 0)

    gather_arrive(2)

    def coarse_step(t, total):
        rows = []
        for k in range(2):
            r = 2 * t + k
            x, y, z = r // (sizes[1] * sizes[2]), r // sizes[2] % sizes[1], r % sizes[2]
            rows.append(
                two[
                    lax.rem(me[0] + x, sizes[0]),
                    lax.rem(me[1] + y, sizes[1]),
                    lax.rem(me[2] + z, sizes[2]),
                ]
            )
        return total + dot(jnp.concatenate(rows, axis=1), coarse_w[t], NT)

    local_two = lax.fori_loop(0, cells // 2, coarse_step, jnp.zeros((half, pts), F32))

    ending(on)

    def far_window(ref, level, e, count):
        ox, oy, oz = (far_offsets[d, level, e] + 2 for d in range(3))
        planes = []
        for i in range(count[0]):
            x = lax.rem(ox + i, ref.shape[0])
            v = ref[x, pl.ds(oy, count[1]), pl.ds(oz, count[2])]
            planes.append(v.reshape(count[1] * count[2] * half, pts))
        return jnp.concatenate(planes, axis=0)

    def far_product(ref, level, t, count):
        rows = [far_window(ref, level, 4 * t + k, count) for k in range(4)]
        return dot(jnp.concatenate(rows, axis=1), far_w[level, t], NT)

    one_acc[...] = jnp.zeros(one_acc.shape, F32)

    def far_one(t, carry):
        one_acc[...] += far_product(one, 1, t, (hx, hy, hz))
        return carry

    lax.fori_loop(0, steps // 4, far_one, 0)

    rounded = local_two.astype(BF16)
    for number in range(8):
        rows = slice(number * half, (number + 1) * half)
        one_acc[rows, :] += dot(rounded, trans_w[number], NN)

    rounded = one_acc[...].astype(BF16)
    for number, (i, j, l) in enumerate(kids):
        value = dot(rounded, trans_w[number], NN)
        for n, (a, b, c) in enumerate(parents):
            box = ((2 * a + i) * by + 2 * b + j) * bz + 2 * c + l
            far_acc[box * half : (box + 1) * half, :] = value[n * half : (n + 1) * half]

    arrive(ch["C"])
    arrive(ch["Cs"])

    def near_side(t, carry):
        near_pair((t - 1, 0, -1), (t - 1, 0, 1))
        return carry

    lax.fori_loop(0, 3, near_side, 0)

    ending(mo)

    def far_zero(t, carry):
        far_acc[...] += far_product(mom, 0, t, (bx, by, bz))
        return carry

    lax.fori_loop(0, steps // 4, far_zero, 0)

    arrive(ch["Cf"])

    def near_corner(t, carry):
        x, y = t // 2 - 1, t % 2 * 2 - 1
        near_pair((x, y, -1), (x, y, 1))
        return carry

    lax.fori_loop(0, 6, near_corner, 0)

    def finish(x, carry):
        span = by * bz * half
        rows = far_acc[pl.ds(pl.multiple_of(x * span, span), span), :].astype(BF16)
        value = dot(rows, basis_w[...], NN)
        for b in range(by * bz):
            y, z = b // bz, b % bz
            live = (lanes < counts[x, y, z]).astype(F32)
            far = jnp.concatenate(
                [
                    value[b * half : (b + 1) * half, 0:pts],
                    value[b * half : (b + 1) * half, pts : 2 * pts],
                ],
                axis=0,
            )
            at = pl.multiple_of((x * by * bz + b) * rhs, rhs)
            out[x, y, z] = (near_acc[pl.ds(at, rhs), :] + far) * live
        return carry

    lax.fori_loop(0, bx, finish, 0)

    groups = list(ch.values()) + list(mo.values()) + list(on.values()) + tw
    for group in groups:
        for c in group:
            c.wait_send()


def body(
    sizes,
    charges,
    counts,
    near_offsets,
    near_blocks,
    leaf_basis,
    transfer,
    far_offsets,
    coupling,
    coarse_coupling,
):
    bx, by, bz, rhs, pts = charges.shape
    half = rhs // 2
    stencil = near_offsets.shape[0]
    boxes = bx * by * bz
    hx, hy, hz = bx // 2, by // 2, bz // 2
    one_x = hx + 2 if sizes[0] * hx == hx + 2 else hx + 4
    levels, steps = coupling.shape[:2]
    cells = sizes[0] * sizes[1] * sizes[2]
    peers = sum(sizes) - 3
    smem = pl.BlockSpec(memory_space=pltpu.SMEM)
    vmem = pl.BlockSpec(memory_space=pltpu.VMEM)
    hbm = pl.BlockSpec(memory_space=pl.ANY)
    return pl.pallas_call(
        functools.partial(kernel, sizes),
        out_shape=jax.ShapeDtypeStruct(charges.shape, F32),
        in_specs=[smem, smem, smem, vmem, vmem, vmem, hbm, hbm, hbm],
        out_specs=vmem,
        scratch_shapes=[
            pltpu.VMEM((bx + 2, by + 2, bz + 2, rhs, pts), BF16),
            pltpu.VMEM((bx + 4, by + 4, bz + 4, half, pts), BF16),
            pltpu.VMEM((one_x, hy + 4, hz + 4, half, pts), BF16),
            pltpu.VMEM(tuple(sizes) + (half, pts), BF16),
            pltpu.VMEM(near_blocks.shape, BF16),
            pltpu.VMEM(coupling.shape, BF16),
            pltpu.VMEM(coarse_coupling.shape, BF16),
            pltpu.VMEM((levels, steps // 4, pts, 4 * pts), BF16),
            pltpu.VMEM((cells // 2, pts, 2 * pts), BF16),
            pltpu.VMEM((8, pts, pts), BF16),
            pltpu.VMEM((pts, 2 * pts), BF16),
            pltpu.VMEM((boxes * rhs, pts), F32),
            pltpu.VMEM((boxes * half, pts), F32),
            pltpu.VMEM((hx * hy * hz * half, pts), F32),
            pltpu.SMEM((stencil,), jnp.int32),
            pltpu.SMEM((stencil,), jnp.int32),
            pltpu.SemaphoreType.DMA((3,)),
            pltpu.SemaphoreType.DMA((54,)),
            pltpu.SemaphoreType.DMA((54,)),
            pltpu.SemaphoreType.DMA((peers,)),
            pltpu.SemaphoreType.DMA((peers,)),
        ],
        compiler_params=pltpu.CompilerParams(
            collective_id=0, has_side_effects=True, vmem_limit_bytes=56 * 1024 * 1024
        ),
    )(
        near_offsets.T,
        counts,
        far_offsets.transpose(2, 0, 1),
        charges,
        leaf_basis,
        transfer,
        near_blocks,
        coupling,
        coarse_coupling,
    )


def solution(mesh):
    sizes = tuple(mesh.shape[a] for a in AXES)
    in_specs = (
        P("gx", "gy", "gz", None, None),
        P("gx", "gy", "gz"),
        P(),
        P(),
        P(),
        P(),
        P(),
        P(),
        P(),
    )
    out_specs = P("gx", "gy", "gz", None, None)
    return jax.shard_map(
        functools.partial(body, sizes),
        mesh=mesh,
        in_specs=in_specs,
        out_specs=out_specs,
        check_vma=False,
    )
```
